256 devices in a mesh: expert: 128 (over y, z, x), tensor: 2 (over core).
Axes of the slice: x: 4, y: 4, z: 8, core: 2. Of those that a mesh axis runs over, the one named last changes fastest.
Arguments:
- states: bfloat16 [16384, 1536], P('expert'), may hold values from -60 to 60
- norm_gain: float32 [1536], replicated, may hold values from 0.25 to 1.75
- router: bfloat16 [1536, 64], replicated, may hold values from -0.15625 to 0.15625
- w_gate: bfloat16 [128, 1536, 2048], P('expert', None, 'tensor'), may hold values from -0.15625 to 0.15625
- w_up: bfloat16 [128, 1536, 2048], P('expert', None, 'tensor'), may hold values from -0.15625 to 0.15625
- w_down: bfloat16 [128, 2048, 1536], P('expert', 'tensor'), may hold values from -0.09375 to 0.09375
- expert_ids: int32 [16384, 2], P('expert'), may hold values from 0 to 63, as said below
- slot_pos: int32 [16384, 2], P('expert'), may hold values from 0 to 6, as said below
- keep_mask: int32 [16384, 2], P('expert'), may hold values from 0 to 1, as said below
Outputs:
- next_states: bfloat16 [16384, 1536], P('expert')
The draws below stay inside these ranges and needn't reach their ends.
Inputs may be any that keep to these rules, and one draw needn't show every extreme that they name: `expert_ids`: each row names two different experts; in every block of 128 rows one expert is named by more than 6 rows. `slot_pos`: for each choice, the number of earlier choices of the same expert within the same block of 128 rows, counted row by row with a row's first choice before its second, or 6 where that number is 6 or more. `keep_mask`: 1 exactly where slot_pos is under 6; in every block of 128 rows some expert has all 6 slots filled.
All inputs are finite; a program needn't handle non-finite values.
Results may differ from the reference program's by a relative error of at most 0.0038.
Values may be sent and summed in bfloat16 or wider, within the bound.
No kernel may reach another device: no remote copies, remote signals or barrier semaphores. Data moves between devices by JAX's collectives and lax.ppermute only.
A program may use at most 64 MiB of HBM per device.

```python
import math
import jax
import jax.numpy as jnp
from jax import lax

D = 1536
FF = 4096
TOP = 2
SHARE = 2
TOK_DEV = 128
EXPERTS = 64
TOKENS = 16384
CAP = 6


def draw_states(key, part):
    keys = jax.random.split(jax.random.fold_in(key, 11), 3)
    row_scale = jnp.exp(jax.random.uniform(keys[0], (TOKENS, 1), minval=math.log(0.3), maxval=math.log(3.0)))
    col_scale = jnp.exp(jax.random.uniform(keys[1], (1, D), minval=math.log(0.4), maxval=math.log(4.0)))
    base = jnp.clip(jax.random.normal(keys[2], (TOKENS, D)), -4.0, 4.0)
    return (base * row_scale * col_scale).astype(jnp.bfloat16)


def routing_tables(key):
    keys = jax.random.split(jax.random.fold_in(key, 7), 5)
    order = jax.random.permutation(keys[0], EXPERTS)
    first_draw = jax.random.randint(keys[1], (TOKENS,), 0, EXPERTS)
    second_draw = jax.random.randint(keys[2], (TOKENS,), 0, EXPERTS)
    first_choice = order[jnp.minimum(first_draw, second_draw)]
    hot_expert = jax.random.randint(keys[3], (), 0, EXPERTS)
    row_in_block = jnp.arange(TOKENS) % TOK_DEV
    first_choice = jnp.where(row_in_block <= CAP, hot_expert, first_choice)
    offsets = jax.random.randint(keys[4], (TOKENS,), 1, EXPERTS)
    second_choice = (first_choice + offsets) % EXPERTS
    chosen_ids = jnp.stack([first_choice, second_choice], axis=1).astype(jnp.int32)
    flat_ids = chosen_ids.reshape(TOKENS // TOK_DEV, TOK_DEV * TOP)
    one_hot = (flat_ids[:, :, None] == jnp.arange(EXPERTS)[None, None, :]).astype(jnp.int32)
    earlier = jnp.cumsum(one_hot, axis=1) - one_hot
    positions = jnp.sum(earlier * one_hot, axis=-1).reshape(TOKENS, TOP).astype(jnp.int32)
    kept_flags = (positions < CAP).astype(jnp.int32)
    positions = jnp.minimum(positions, CAP).astype(jnp.int32)
    return (chosen_ids, positions, kept_flags)


def draw_expert_ids(key, part):
    return routing_tables(key)[0]


def draw_slot_pos(key, part):
    return routing_tables(key)[1]


def draw_keep_mask(key, part):
    return routing_tables(key)[2]


def shard_levels(rng, shape, pieces, least, largest):
    level, own = 1.0, jax.random.fold_in(rng, 6)
    for axis_at, parts in pieces:
        steps = jnp.exp(jax.random.uniform(jax.random.fold_in(own, axis_at), (parts,), jnp.float32, least / len(pieces), largest / len(pieces)))
        level = level * jnp.repeat(steps, shape[axis_at] // parts).reshape([-1 if axis == axis_at else 1 for axis in range(len(shape))])
    return level


def normal_values(stream_key, dims, spread, bound, pieces=(), dtype=jnp.bfloat16):
    array = spread * jax.random.normal(stream_key, dims, jnp.float32)
    if pieces:
        array = array * shard_levels(stream_key, dims, pieces, -0.22, 0.18)
    return jnp.clip(array, -bound, bound).astype(dtype)


def setup_inputs(seed: int = 0) -> dict:
    arg_keys = jax.random.split(jax.random.key(seed), 10)
    return {
        "states": draw_states(jax.random.fold_in(arg_keys[9], 71), 0),
        "norm_gain": jnp.clip(1.0 + 0.15 * jax.random.normal(arg_keys[1], (D,), jnp.float32), 0.25, 1.75),
        "router": normal_values(arg_keys[2], (D, EXPERTS), D ** -0.5, 0.15625),
        "w_gate": normal_values(arg_keys[3], (EXPERTS * SHARE, D, FF // SHARE), D ** -0.5, 0.15625, ((0, 128), (2, 2))),
        "w_up": normal_values(arg_keys[4], (EXPERTS * SHARE, D, FF // SHARE), D ** -0.5, 0.15625, ((0, 128), (2, 2))),
        "w_down": normal_values(arg_keys[5], (EXPERTS * SHARE, FF // SHARE, D), FF ** -0.5, 0.09375, ((0, 128), (1, 2))),
        "expert_ids": draw_expert_ids(jax.random.fold_in(arg_keys[9], 71), 0),
        "slot_pos": draw_slot_pos(jax.random.fold_in(arg_keys[9], 71), 0),
        "keep_mask": draw_keep_mask(jax.random.fold_in(arg_keys[9], 71), 0),
    }


def expert_ffn(operands):
    slot_rows, gate_parts, up_parts, down_parts = operands
    gate_mat = jnp.concatenate([gate_parts[h] for h in range(SHARE)], axis=1)
    up_mat = jnp.concatenate([up_parts[h] for h in range(SHARE)], axis=1)
    down_mat = down_parts.reshape(FF, D)
    flat_rows = slot_rows.reshape(-1, D)
    gate_act = jnp.dot(flat_rows, gate_mat, preferred_element_type=jnp.float32)
    up_act = jnp.dot(flat_rows, up_mat, preferred_element_type=jnp.float32)
    hidden = (jax.nn.silu(gate_act) * up_act).astype(jnp.bfloat16)
    result = jnp.dot(hidden, down_mat, preferred_element_type=jnp.float32).astype(jnp.bfloat16)
    return result.reshape(slot_rows.shape)

def reference(states, norm_gain, router, w_gate, w_up, w_down, expert_ids, slot_pos, keep_mask):
    values = states.astype(jnp.float32)
    normed = (values * lax.rsqrt(lax.optimization_barrier(jnp.mean(values * values, axis=-1, keepdims=True)) + 1e-06) * norm_gain).astype(jnp.bfloat16)
    logits = jnp.dot(normed, router, preferred_element_type=jnp.float32)
    chosen = jnp.take_along_axis(logits, expert_ids, axis=1)
    gate_score = jax.nn.sigmoid(chosen)
    weight = gate_score / lax.optimization_barrier(jnp.sum(gate_score, axis=1, keepdims=True))
    num_blocks = TOKENS // TOK_DEV
    block_id = (jnp.arange(TOKENS) // TOK_DEV).astype(jnp.int32)
    is_kept = keep_mask > 0
    target_expert = jnp.where(is_kept, expert_ids, EXPERTS).astype(jnp.int32)
    block_index = jnp.broadcast_to(block_id[:, None], expert_ids.shape)
    updates = jnp.broadcast_to(normed[:, None, :], (TOKENS, TOP, D))
    slot_buffer = jnp.zeros((EXPERTS, num_blocks, CAP, D), jnp.bfloat16)
    slot_buffer = slot_buffer.at[target_expert, block_index, slot_pos].set(updates, mode='drop')
    gate_split = w_gate.reshape(EXPERTS, SHARE, D, FF // SHARE)
    up_split = w_up.reshape(EXPERTS, SHARE, D, FF // SHARE)
    down_split = w_down.reshape(EXPERTS, SHARE, FF // SHARE, D)
    expert_out = lax.map(expert_ffn, (slot_buffer, gate_split, up_split, down_split))
    safe_pos = jnp.minimum(slot_pos, CAP - 1).astype(jnp.int32)
    picked = expert_out[expert_ids, block_index, safe_pos].astype(jnp.float32)
    factor = jnp.where(is_kept, weight, 0.0).astype(jnp.float32)
    combined = lax.optimization_barrier(jnp.sum(factor[:, :, None] * picked, axis=1))
    return (values + combined).astype(jnp.bfloat16)
```

```python
import jax
import jax.numpy as jnp
from jax import lax
from jax.sharding import PartitionSpec as P

CHUNKS = ((0, 1, 2),)
SWAP = ((0, 1), (1, 0))


def swap(x):
    return lax.ppermute(x, "tensor", SWAP)


def dot(a, b):
    return jnp.dot(a, b, preferred_element_type=jnp.float32)


def per_device(states, norm_gain, router, w_gate, w_up, w_down, expert_ids, slot_pos, keep_mask):
    tok_rows, width = states.shape
    groups = lax.axis_size("expert")
    all_experts = router.shape[1]
    holders = groups // all_experts
    capacity = max(2, 5 * tok_rows // (2 * all_experts) + 1)
    own_slots = capacity // 2
    first_slot = lax.axis_index("tensor") * own_slots

    gates = (w_gate[0], swap(w_gate)[0])
    ups = (w_up[0], swap(w_up)[0])
    downs = (w_down[0], swap(w_down)[0])

    values = states.astype(jnp.float32)
    normed = (
        values * lax.rsqrt(jnp.mean(values * values, axis=-1, keepdims=True) + 1e-06) * norm_gain
    ).astype(jnp.bfloat16)
    is_kept = keep_mask > 0
    slot_index = jnp.where(is_kept, expert_ids * capacity + slot_pos, -1)
    key = lax.broadcasted_iota(jnp.int32, (groups, tok_rows), 0) // holders * capacity + first_slot

    def send(chunk):
        rows = []
        for j in chunk:
            hit = (key + j == slot_index[:, 0][None, :]) | (key + j == slot_index[:, 1][None, :])
            rows.append(dot(hit.astype(jnp.bfloat16), normed).astype(jnp.bfloat16))
        rows = jnp.concatenate(rows, axis=1)
        return lax.all_to_all(rows, "expert", 0, 0, tiled=True)

    def ffn(arrived, chunk):
        rows = jnp.concatenate(
            [arrived[:, n * width : (n + 1) * width] for n in range(len(chunk))], axis=0
        )
        total = 0.0
        for g, u, d in zip(gates, ups, downs):
            hidden = (jax.nn.silu(dot(rows, g)) * dot(rows, u)).astype(jnp.bfloat16)
            total = total + dot(hidden, d)
        total = total.astype(jnp.bfloat16)
        back = jnp.concatenate(
            [total[n * groups : (n + 1) * groups] for n in range(len(chunk))], axis=1
        )
        return lax.all_to_all(back, "expert", 0, 0, tiled=True)

    arrived = [send(c) for c in CHUNKS]

    logits = dot(normed, router)
    columns = lax.broadcasted_iota(jnp.int32, (tok_rows, all_experts), 1)
    chosen = jnp.stack(
        [
            jnp.sum(jnp.where(columns == expert_ids[:, pick][:, None], logits, 0.0), axis=1)
            for pick in range(2)
        ],
        axis=1,
    )
    gate_score = jax.nn.sigmoid(chosen)
    weight = gate_score / jnp.sum(gate_score, axis=1, keepdims=True)
    key_t = lax.broadcasted_iota(jnp.int32, (tok_rows, groups), 1) // holders * capacity + first_slot

    returned = [ffn(a, c) for a, c in zip(arrived, CHUNKS)]

    partial = 0.0
    for back, chunk in zip(returned, CHUNKS):
        for n, j in enumerate(chunk):
            share = sum(
                jnp.where(key_t + j == slot_index[:, k][:, None], weight[:, k][:, None], 0.0)
                for k in range(2)
            )
            high = lax.reduce_precision(share, 8, 7)
            low = (share - high).astype(jnp.bfloat16)
            rows = back[:, n * width : (n + 1) * width]
            partial = partial + dot(high.astype(jnp.bfloat16), rows) + dot(low, rows)
    mine = partial.astype(jnp.bfloat16)
    other = swap(mine)
    mine = lax.reduce_precision(partial, 8, 7)
    return (values + (mine + other.astype(jnp.float32))).astype(jnp.bfloat16)


def solution(mesh):
    placed = (
        P("expert", None),
        P(),
        P(),
        P("expert", None, "tensor"),
        P("expert", None, "tensor"),
        P("expert", "tensor", None),
        P("expert", None),
        P("expert", None),
        P("expert", None),
    )
    return jax.shard_map(
        per_device, mesh=mesh, in_specs=placed, out_specs=P("expert", None), check_vma=False
    )
```

```python
import functools

import jax
import jax.numpy as jnp
from jax import lax
from jax.experimental import pallas as pl
from jax.experimental.pallas import tpu as pltpu
from jax.sharding import PartitionSpec as P

SWAP = ((0, 1), (1, 0))
MIB = 1 << 20
BF16 = jnp.bfloat16
F32 = jnp.float32
VMEM = pl.BlockSpec(memory_space=pltpu.VMEM)
ANY = pl.BlockSpec(memory_space=pl.ANY)


def swap(x):
    return lax.ppermute(x, "tensor", SWAP)


def dot(a, b):
    return jnp.dot(a, b, preferred_element_type=F32)


def dispatch_kernel(first, holders, capacity, slots_own, states, gain, slots, normed_out, send):
    rows, width = states.shape
    groups = send.shape[0]
    values = states[...].astype(F32)
    mean = jnp.mean(values * values, axis=-1, keepdims=True)
    normed = (values * lax.rsqrt(mean + 1e-06) * gain[...]).astype(BF16)
    normed_out[...] = normed
    owner = lax.broadcasted_iota(jnp.int32, (groups, rows), 0) // holders * capacity
    half = width // 2
    for j in range(slots_own):
        key = owner + (first[0] + j)
        hit = (key == slots[0:1, :]) | (key == slots[1:2, :])
        moved = dot(jnp.where(hit, 1.0, 0.0).astype(BF16), normed).astype(BF16)
        send[:, :, j * half : (j + 1) * half] = moved.reshape(groups, 2, half)


def weights_kernel(first, holders, capacity, slots_own, normed, router, ids, slots, table):
    rows = normed.shape[0]
    experts = router.shape[0]
    groups = experts * holders
    logits = lax.dot_general(
        router[...], normed[...], (((1,), (1,)), ((), ())), preferred_element_type=F32
    )
    expert = lax.broadcasted_iota(jnp.int32, (experts, rows), 0)
    score = []
    for k in range(2):
        chosen = jnp.sum(jnp.where(expert == ids[k : k + 1, :], logits, 0.0), axis=0, keepdims=True)
        score.append(1.0 / (1.0 + jnp.exp(-chosen)))
    total = score[0] + score[1]
    owner = lax.broadcasted_iota(jnp.int32, (groups, rows), 0) // holders * capacity
    for j in range(slots_own):
        key = owner + (first[0] + j)
        share = jnp.where(key == slots[0:1, :], score[0] / total, 0.0)
        share = share + jnp.where(key == slots[1:2, :], score[1] / total, 0.0)
        share = share.T
        high = share.astype(BF16)
        low = (share - high.astype(F32)).astype(BF16)
        table[:, (2 * j) * groups : (2 * j + 1) * groups] = high
        table[:, (2 * j + 1) * groups : (2 * j + 2) * groups] = low


def expert_kernel(slots_own, arrived, *refs):
    hbm, (back, rows, hidden, out, gates, ups, downs, sems) = refs[:6], refs[6:]
    groups = arrived.shape[0]
    width = rows.shape[1]
    part = gates.shape[2]
    piece = part // 2
    half = width // 2
    copies = []

    def start(src, dst):
        copy = pltpu.make_async_copy(src, dst, sems.at[len(copies)])
        copy.start()
        copies.append(copy)
        return copy

    loads = []
    for s in range(2):
        for p in range(2):
            cols = slice(p * piece, (p + 1) * piece)
            g = start(hbm[3 * s].at[:, cols], gates.at[s, :, cols])
            u = start(hbm[3 * s + 1].at[:, cols], ups.at[s, :, cols])
            loads.append((g, u))
    down_loads = [start(hbm[3 * s + 2], downs.at[s]) for s in range(2)]
    for j in range(slots_own):
        rows[j * groups : (j + 1) * groups, :] = arrived[:, :, j * half : (j + 1) * half].reshape(
            groups, width
        )
    for s in range(2):
        for p in range(2):
            for copy in loads[2 * s + p]:
                copy.wait()
            for q in range(piece // 256):
                lo = p * piece + q * 256
                gate = dot(rows[...], gates[s, :, lo : lo + 256])
                up = dot(rows[...], ups[s, :, lo : lo + 256])
                hidden[:, s * part + lo : s * part + lo + 256] = (
                    gate / (1.0 + jnp.exp(-gate)) * up
                ).astype(BF16)
    for copy in down_loads:
        copy.wait()
    for n in range(width // 256):
        cols = slice(n * 256, (n + 1) * 256)
        total = dot(hidden[:, :part], downs[0, :, cols]) + dot(hidden[:, part:], downs[1, :, cols])
        out[:, cols] = total.astype(BF16)
    for j in range(slots_own):
        back[:, :, j * half : (j + 1) * half] = out[j * groups : (j + 1) * groups, :].reshape(
            groups, 2, half
        )


def combine_kernel(slots_own, table, returned, partial):
    groups = returned.shape[0]
    width = partial.shape[1]
    half = width // 2
    total = jnp.zeros(partial.shape, F32)
    for j in range(slots_own):
        rows = returned[:, :, j * half : (j + 1) * half].reshape(groups, width)
        high = table[:, (2 * j) * groups : (2 * j + 1) * groups]
        low = table[:, (2 * j + 1) * groups : (2 * j + 2) * groups]
        total = total + dot(high, rows) + dot(low, rows)
    partial[...] = total.astype(BF16)


def per_device(states, norm_gain, router, w_gate, w_up, w_down, expert_ids, slot_pos, keep_mask):
    rows, width = states.shape
    groups = lax.axis_size("expert")
    experts = router.shape[1]
    holders = groups // experts
    capacity = max(2, 5 * rows // (2 * experts) + 1)
    own = capacity // 2
    part = w_gate.shape[2]
    first = (lax.axis_index("tensor") * own).astype(jnp.int32).reshape(1)
    smem = pl.BlockSpec(memory_space=pltpu.SMEM)
    mine = (w_gate[0], w_up[0], w_down[0])
    theirs = tuple(swap(w)[0] for w in (w_gate, w_up, w_down))
    ids = expert_ids.T
    slots = jnp.where(keep_mask.T > 0, ids * capacity + slot_pos.T, -1)

    packet = jax.ShapeDtypeStruct((groups, 2, own * width // 2), BF16)
    normed, send = pl.pallas_call(
        lambda *refs: dispatch_kernel(refs[0], holders, capacity, own, *refs[1:]),
        out_shape=(jax.ShapeDtypeStruct(states.shape, BF16), packet),
        in_specs=[smem, VMEM, VMEM, VMEM],
        out_specs=(VMEM, VMEM),
        compiler_params=pltpu.CompilerParams(vmem_limit_bytes=24 * MIB),
        name="dispatch",
    )(first, states, norm_gain[None, :], slots)
    arrived = lax.all_to_all(send, "expert", 0, 0, tiled=True)
    table = pl.pallas_call(
        lambda *refs: weights_kernel(refs[0], holders, capacity, own, *refs[1:]),
        out_shape=jax.ShapeDtypeStruct((rows, own * 2 * groups), BF16),
        in_specs=[smem, VMEM, VMEM, VMEM, VMEM],
        out_specs=VMEM,
        compiler_params=pltpu.CompilerParams(vmem_limit_bytes=16 * MIB),
        cost_estimate=pl.CostEstimate(flops=2 * 10**9, bytes_accessed=10**6, transcendentals=0),
        name="weights",
    )(first, normed, router.T, ids, slots)
    back = pl.pallas_call(
        functools.partial(expert_kernel, own),
        out_shape=packet,
        in_specs=[VMEM] + [ANY] * 6,
        out_specs=VMEM,
        scratch_shapes=[
            pltpu.VMEM((own * groups, width), BF16),
            pltpu.VMEM((own * groups, 2 * part), BF16),
            pltpu.VMEM((own * groups, width), BF16),
            pltpu.VMEM((2, width, part), BF16),
            pltpu.VMEM((2, width, part), BF16),
            pltpu.VMEM((2, part, width), BF16),
            pltpu.SemaphoreType.DMA((10,)),
        ],
        compiler_params=pltpu.CompilerParams(vmem_limit_bytes=60 * MIB),
        cost_estimate=pl.CostEstimate(
            flops=12 * own * groups * width * part, bytes_accessed=20 * 10**6, transcendentals=0
        ),
        name="experts",
    )(arrived, *mine, *theirs)
    returned = lax.all_to_all(back, "expert", 0, 0, tiled=True)
    partial = pl.pallas_call(
        functools.partial(combine_kernel, own),
        out_shape=jax.ShapeDtypeStruct(states.shape, BF16),
        in_specs=[VMEM, VMEM],
        out_specs=VMEM,
        compiler_params=pltpu.CompilerParams(vmem_limit_bytes=16 * MIB),
        name="combine",
    )(table, returned)
    added = partial.astype(F32) + swap(partial).astype(F32)
    return (states.astype(F32) + added).astype(BF16)


def solution(mesh):
    placed = (
        P("expert", None),
        P(),
        P(),
        P("expert", None, "tensor"),
        P("expert", None, "tensor"),
        P("expert", "tensor", None),
        P("expert", None),
        P("expert", None),
        P("expert", None),
    )
    return jax.shard_map(
        per_device, mesh=mesh, in_specs=placed, out_specs=P("expert", None), check_vma=False
    )
```

```python
import functools

import jax
import jax.numpy as jnp
from jax import lax
from jax.experimental import pallas as pl
from jax.experimental.pallas import tpu as pltpu
from jax.sharding import Mesh, PartitionSpec as P

SWAP = ((0, 1), (1, 0))
AXES = (4, 8, 4)
MIB = 1 << 20
BF16 = jnp.bfloat16
F32 = jnp.float32
VMEM = pl.BlockSpec(memory_space=pltpu.VMEM)
ANY = pl.BlockSpec(memory_space=pl.ANY)


def swap(x):
    return lax.ppermute(x, "tensor", SWAP)


def dot(a, b):
    return jnp.dot(a, b, preferred_element_type=F32)


def iota(shape, dim):
    return lax.broadcasted_iota(jnp.int32, shape, dim)


def slot_keys(own, tokens):
    ys, zs, xs = AXES
    pairs = xs // 2
    shape = (zs, own, ys * pairs, tokens)
    inner = iota(shape, 2)
    expert = (inner // pairs * zs + iota(shape, 0)) * pairs + inner % pairs
    key = expert * (2 * own) + iota(shape, 1) + lax.axis_index("tensor") * own
    return key.reshape(zs * own * ys * pairs, tokens)


def slot_numbers(own, ids, pos, keep):
    return jnp.where(keep[...] > 0, ids[...] * (2 * own) + pos[...], -1)


def dispatch_kernel(own, states, gain, ids, pos, keep, normed_out, send):
    tokens = states.shape[0]
    values = states[...].astype(F32)
    mean = jnp.mean(values * values, axis=-1, keepdims=True)
    normed = (values * lax.rsqrt(mean + 1e-06) * gain[...][None, :]).astype(BF16)
    normed_out[...] = normed
    slots = slot_numbers(own, ids, pos, keep)
    key = slot_keys(own, tokens)
    hit = (key == slots[0:1, :]) | (key == slots[1:2, :])
    send[...] = dot(jnp.where(hit, 1.0, 0.0).astype(BF16), normed).astype(BF16)


def regroup_kernel(own, arrived, send):
    ys, zs, xs = AXES
    experts = ys * xs // 2
    count = experts * own * zs
    shape = (experts, own, zs, count)
    source = (iota(shape, 2) * own + iota(shape, 1)) * experts + iota(shape, 0)
    pick = (source == iota(shape, 3)).reshape(count, count)
    rows = dot(jnp.where(pick, 1.0, 0.0).astype(BF16), arrived[...]).astype(BF16)
    size = own * zs
    for e in range(experts):
        for h in range(2):
            send[(2 * e + h) * size : (2 * e + h + 1) * size, :] = rows[e * size : (e + 1) * size, :]


def gather_kernel(own, partial, send):
    ys, zs, xs = AXES
    experts = ys * xs // 2
    count = experts * own * zs
    shape = (zs, own, experts, 2 * count)
    holder = (iota(shape, 2) * 2 * own + iota(shape, 1)) * zs + iota(shape, 0)
    column = iota(shape, 3)
    pick = ((column == holder) | (column == holder + own * zs)).reshape(count, 2 * count)
    send[...] = dot(jnp.where(pick, 1.0, 0.0).astype(BF16), partial[...]).astype(BF16)


def weights_kernel(own, normed, router, ids, pos, keep, table):
    tokens = normed.shape[0]
    experts = router.shape[0]
    logits = lax.dot_general(
        router[...], normed[...], (((1,), (1,)), ((), ())), preferred_element_type=F32
    )
    expert = iota((experts, tokens), 0)
    score = []
    for k in range(2):
        chosen = jnp.sum(jnp.where(expert == ids[k : k + 1, :], logits, 0.0), axis=0, keepdims=True)
        score.append(1.0 / (1.0 + jnp.exp(-chosen)))
    total = score[0] + score[1]
    slots = slot_numbers(own, ids, pos, keep)
    key = slot_keys(own, tokens)
    share = jnp.where(key == slots[0:1, :], score[0] / total, 0.0)
    share = share + jnp.where(key == slots[1:2, :], score[1] / total, 0.0)
    share = share.T
    high = share.astype(BF16)
    table[0] = high
    table[1] = (share - high.astype(F32)).astype(BF16)


def expert_kernel(rows, *refs):
    hbm, (back, hidden, gates, ups, downs, sems) = refs[:6], refs[6:]
    width = rows.shape[1]
    part = gates.shape[2]
    piece = part // 2
    copies = []

    def start(src, dst):
        copy = pltpu.make_async_copy(src, dst, sems.at[len(copies)])
        copy.start()
        copies.append(copy)
        return copy

    loads = []
    for s in range(2):
        for p in range(2):
            cols = slice(p * piece, (p + 1) * piece)
            g = start(hbm[3 * s].at[:, cols], gates.at[s, :, cols])
            u = start(hbm[3 * s + 1].at[:, cols], ups.at[s, :, cols])
            loads.append((g, u))
    down_loads = [
        start(hbm[3 * s + 2], downs.at[s * part : (s + 1) * part, :]) for s in range(2)
    ]
    for s in range(2):
        for p in range(2):
            for copy in loads[2 * s + p]:
                copy.wait()
            cols = slice(p * piece, (p + 1) * piece)
            gate = dot(rows[...], gates[s, :, cols])
            up = dot(rows[...], ups[s, :, cols])
            hidden[:, s * part + p * piece : s * part + (p + 1) * piece] = (
                gate / (1.0 + jnp.exp(-gate)) * up
            ).astype(BF16)
    for copy in down_loads:
        copy.wait()
    for n in range(width // 512):
        cols = slice(n * 512, (n + 1) * 512)
        back[:, cols] = dot(hidden[...], downs[:, cols]).astype(BF16)


def combine_kernel(table, returned, partial):
    partial[...] = (dot(table[0], returned[...]) + dot(table[1], returned[...])).astype(BF16)


def params(mib):
    return pltpu.CompilerParams(vmem_limit_bytes=mib * MIB)


def per_device(states, norm_gain, router, w_gate, w_up, w_down, expert_ids, slot_pos, keep_mask):
    tokens, width = states.shape
    ys, zs, xs = AXES
    experts = router.shape[1]
    own = max(2, 5 * tokens // (2 * experts) + 1) // 2
    part = w_gate.shape[2]
    chips = ys * xs
    once = own * experts
    rows = jax.ShapeDtypeStruct((once, width), BF16)
    twice = jax.ShapeDtypeStruct((2 * once, width), BF16)
    mine = (w_gate[0], w_up[0], w_down[0])
    theirs = tuple(swap(w)[0] for w in (w_gate, w_up, w_down))
    routing = (expert_ids.T, slot_pos.T, keep_mask.T)

    def along_z(x):
        x = x.reshape(zs, once // zs, width)
        return lax.all_to_all(x, "z", 0, 0, tiled=True).reshape(once, width)

    def in_plane(x):
        x = x.reshape(chips, 2 * once // chips, width)
        return lax.all_to_all(x, ("y", "x"), 0, 0, tiled=True).reshape(2 * once, width)

    normed, send = pl.pallas_call(
        functools.partial(dispatch_kernel, own),
        out_shape=(jax.ShapeDtypeStruct(states.shape, BF16), rows),
        in_specs=[VMEM] * 5,
        out_specs=(VMEM, VMEM),
        compiler_params=params(16),
        name="dispatch",
    )(states, norm_gain, *routing)
    column = along_z(send)
    table = pl.pallas_call(
        functools.partial(weights_kernel, own),
        out_shape=jax.ShapeDtypeStruct((2, tokens, once), BF16),
        in_specs=[VMEM] * 5,
        out_specs=VMEM,
        compiler_params=params(16),
        cost_estimate=pl.CostEstimate(flops=2 * 10**9, bytes_accessed=10**6, transcendentals=0),
        name="weights",
    )(normed, router.T, *routing)
    spread = pl.pallas_call(
        functools.partial(regroup_kernel, own),
        out_shape=twice,
        in_specs=[VMEM],
        out_specs=VMEM,
        compiler_params=params(16),
        name="regroup",
    )(column)
    arrived = in_plane(spread)
    back = pl.pallas_call(
        expert_kernel,
        out_shape=twice,
        in_specs=[VMEM] + [ANY] * 6,
        out_specs=VMEM,
        scratch_shapes=[
            pltpu.VMEM((2 * once, 2 * part), BF16),
            pltpu.VMEM((2, width, part), BF16),
            pltpu.VMEM((2, width, part), BF16),
            pltpu.VMEM((2 * part, width), BF16),
            pltpu.SemaphoreType.DMA((10,)),
        ],
        compiler_params=params(60),
        cost_estimate=pl.CostEstimate(
            flops=24 * once * width * part, bytes_accessed=20 * 10**6, transcendentals=0
        ),
        name="experts",
    )(arrived, *mine, *theirs)
    plane = in_plane(back)
    summed = pl.pallas_call(
        functools.partial(gather_kernel, own),
        out_shape=rows,
        in_specs=[VMEM],
        out_specs=VMEM,
        compiler_params=params(16),
        name="gather",
    )(plane)
    returned = along_z(summed)
    partial = pl.pallas_call(
        combine_kernel,
        out_shape=jax.ShapeDtypeStruct(states.shape, BF16),
        in_specs=[VMEM, VMEM],
        out_specs=VMEM,
        compiler_params=params(16),
        name="combine",
    )(table, returned)
    added = partial.astype(F32) + swap(partial).astype(F32)
    return (states.astype(F32) + added).astype(BF16)


def solution(mesh):
    grid = Mesh(mesh.devices.reshape(*AXES, 2), ("y", "z", "x", "tensor"))
    group = ("y", "z", "x")
    placed = (
        P(group, None),
        P(),
        P(),
        P(group, None, "tensor"),
        P(group, None, "tensor"),
        P(group, "tensor", None),
        P(group, None),
        P(group, None),
        P(group, None),
    )
    return jax.shard_map(
        per_device, mesh=grid, in_specs=placed, out_specs=P(group, None), check_vma=False
    )
```

```python
import functools

import jax
import jax.numpy as jnp
from jax import lax
from jax.experimental import pallas as pl
from jax.experimental.pallas import tpu as pltpu
from jax.sharding import Mesh, PartitionSpec as P

SWAP = ((0, 1), (1, 0))
AXES = (4, 8, 4)
MIB = 1 << 20
BF16 = jnp.bfloat16
F32 = jnp.float32
VMEM = pl.BlockSpec(memory_space=pltpu.VMEM)
ANY = pl.BlockSpec(memory_space=pl.ANY)


def swap(x):
    return lax.ppermute(x, "tensor", SWAP)


def dot(a, b):
    return jnp.dot(a, b, preferred_element_type=F32)


def iota(shape, dim):
    return lax.broadcasted_iota(jnp.int32, shape, dim)


def slot_keys(own, tokens):
    ys, zs, xs = AXES
    pairs = xs // 2
    shape = (zs, own, ys * pairs, tokens)
    inner = iota(shape, 2)
    expert = (inner // pairs * zs + iota(shape, 0)) * pairs + inner % pairs
    key = expert * (2 * own) + iota(shape, 1) + lax.axis_index("tensor") * own
    return key.reshape(zs * own * ys * pairs, tokens)


def slot_numbers(own, ids, pos, keep):
    return jnp.where(keep[...] > 0, ids[...] * (2 * own) + pos[...], -1)


def dispatch_kernel(own, *refs):
    sources, (normed_out, send), targets, sems = refs[:5], refs[5:7], refs[7:12], refs[12]
    copies = [
        pltpu.make_async_copy(source, target, sems.at[n])
        for n, (source, target) in enumerate(zip(sources, targets))
    ]
    for copy in copies:
        copy.start()
    states, gain, ids, pos, keep = targets
    tokens = states.shape[0]
    for copy in copies[2:]:
        copy.wait()
    slots = slot_numbers(own, ids, pos, keep)
    key = slot_keys(own, tokens)
    hit = (key == slots[0:1, :]) | (key == slots[1:2, :])
    pick = jnp.where(hit, 1.0, 0.0).astype(BF16)
    for copy in copies[:2]:
        copy.wait()
    values = states[...].astype(F32)
    mean = jnp.mean(values * values, axis=-1, keepdims=True)
    normed = (values * lax.rsqrt(mean + 1e-06) * gain[...][None, :]).astype(BF16)
    normed_out[...] = normed
    send[...] = dot(pick, normed).astype(BF16)


def regroup_kernel(own, arrived, send):
    ys, zs, xs = AXES
    experts = ys * xs // 2
    count = experts * own * zs
    shape = (experts, own, zs, count)
    source = (iota(shape, 2) * own + iota(shape, 1)) * experts + iota(shape, 0)
    pick = (source == iota(shape, 3)).reshape(count, count)
    rows = dot(jnp.where(pick, 1.0, 0.0).astype(BF16), arrived[...]).astype(BF16)
    size = own * zs
    for e in range(experts):
        for h in range(2):
            send[(2 * e + h) * size : (2 * e + h + 1) * size, :] = rows[e * size : (e + 1) * size, :]


def gather_kernel(own, partial, send):
    ys, zs, xs = AXES
    experts = ys * xs // 2
    count = experts * own * zs
    shape = (zs, own, experts, 2 * count)
    holder = (iota(shape, 2) * 2 * own + iota(shape, 1)) * zs + iota(shape, 0)
    column = iota(shape, 3)
    pick = ((column == holder) | (column == holder + own * zs)).reshape(count, 2 * count)
    send[...] = dot(jnp.where(pick, 1.0, 0.0).astype(BF16), partial[...]).astype(BF16)


def weigh(own, normed, router, ids, pos, keep, table):
    tokens = normed.shape[0]
    experts = router.shape[0]
    logits = lax.dot_general(
        router[...], normed[...], (((1,), (1,)), ((), ())), preferred_element_type=F32
    )
    expert = iota((experts, tokens), 0)
    score = []
    for k in range(2):
        chosen = jnp.sum(jnp.where(expert == ids[k : k + 1, :], logits, 0.0), axis=0, keepdims=True)
        score.append(1.0 / (1.0 + jnp.exp(-chosen)))
    total = score[0] + score[1]
    slots = slot_numbers(own, ids, pos, keep)
    key = slot_keys(own, tokens)
    share = jnp.where(key == slots[0:1, :], score[0] / total, 0.0)
    share = share + jnp.where(key == slots[1:2, :], score[1] / total, 0.0)
    share = share.T
    high = share.astype(BF16)
    table[0] = high
    table[1] = (share - high.astype(F32)).astype(BF16)


def expert_kernel(own, rows, *refs):
    theirs, gate_mine, distant, routing = refs[:3], refs[3], refs[4:6], refs[6:11]
    back, table, hidden, up_mine, down_mine, sems = refs[11:]
    width = rows.shape[1]
    part = gate_mine.shape[1]
    block = 512
    copies = [
        pltpu.make_async_copy(source, target, sems.at[n])
        for n, (source, target) in enumerate(zip(distant, (up_mine, down_mine)))
    ]
    for copy in copies:
        copy.start()
    weigh(own, *routing, table)

    def hide(gates, ups, at):
        for n in range(part // block):
            cols = slice(n * block, (n + 1) * block)
            gate = dot(rows[...], gates[:, cols])
            up = dot(rows[...], ups[:, cols])
            hidden[:, at + n * block : at + (n + 1) * block] = (
                gate / (1.0 + jnp.exp(-gate)) * up
            ).astype(BF16)

    hide(theirs[0], theirs[1], 0)
    copies[0].wait()
    hide(gate_mine, up_mine, part)
    copies[1].wait()
    for n in range(width // block):
        cols = slice(n * block, (n + 1) * block)
        total = dot(hidden[:, :part], theirs[2][:, cols])
        total = total + dot(hidden[:, part:], down_mine[:, cols])
        back[:, cols] = total.astype(BF16)


def combine_kernel(table, returned, partial):
    partial[...] = (dot(table[0], returned[...]) + dot(table[1], returned[...])).astype(BF16)


def near(x):
    return pltpu.with_memory_space_constraint(x, pltpu.VMEM)


def far(x):
    return pltpu.with_memory_space_constraint(x, pltpu.HBM)


def params(mib):
    return pltpu.CompilerParams(vmem_limit_bytes=mib * MIB)


def per_device(states, norm_gain, router, w_gate, w_up, w_down, expert_ids, slot_pos, keep_mask):
    tokens, width = states.shape
    ys, zs, xs = AXES
    experts = router.shape[1]
    own = max(2, 5 * tokens // (2 * experts) + 1) // 2
    part = w_gate.shape[2]
    chips = ys * xs
    once = own * experts
    rows = pltpu.VMEM((once, width), BF16)
    twice = pltpu.VMEM((2 * once, width), BF16)
    mine = (w_gate[0], w_up[0], w_down[0])
    theirs = tuple(swap(w)[0] for w in (w_gate, w_up, w_down))
    routing = (expert_ids.T, slot_pos.T, keep_mask.T)

    def along_z(x):
        x = x.reshape(zs, once // zs, width)
        return near(lax.all_to_all(x, "z", 0, 0, tiled=True).reshape(once, width))

    def in_plane(x):
        x = x.reshape(chips, 2 * once // chips, width)
        x = lax.all_to_all(x, ("y", "x"), 0, 0, tiled=True)
        return near(x.reshape(2 * once, width))

    loaded = (states, norm_gain, *routing)
    normed, send = pl.pallas_call(
        functools.partial(dispatch_kernel, own),
        out_shape=(pltpu.VMEM(states.shape, BF16), rows),
        in_specs=[ANY] * 5,
        out_specs=(VMEM, VMEM),
        scratch_shapes=[pltpu.VMEM(x.shape, x.dtype) for x in loaded]
        + [pltpu.SemaphoreType.DMA((5,))],
        compiler_params=params(16),
        name="dispatch",
    )(*map(far, loaded))
    spread = pl.pallas_call(
        functools.partial(regroup_kernel, own),
        out_shape=twice,
        in_specs=[VMEM],
        out_specs=VMEM,
        compiler_params=params(16),
        name="regroup",
    )(along_z(send))
    back, table = pl.pallas_call(
        functools.partial(expert_kernel, own),
        out_shape=(twice, pltpu.VMEM((2, tokens, once), BF16)),
        in_specs=[VMEM] * 5 + [ANY] * 2 + [VMEM] * 5,
        out_specs=(VMEM, VMEM),
        scratch_shapes=[
            pltpu.VMEM((2 * once, 2 * part), BF16),
            pltpu.VMEM((width, part), BF16),
            pltpu.VMEM((part, width), BF16),
            pltpu.SemaphoreType.DMA((2,)),
        ],
        compiler_params=params(40),
        cost_estimate=pl.CostEstimate(
            flops=24 * once * width * part, bytes_accessed=20 * 10**6, transcendentals=0
        ),
        name="experts",
    )(
        in_plane(spread),
        *map(near, theirs + mine[:1]),
        *map(far, mine[1:]),
        near(normed),
        router.T,
        *routing,
    )
    summed = pl.pallas_call(
        functools.partial(gather_kernel, own),
        out_shape=rows,
        in_specs=[VMEM],
        out_specs=VMEM,
        compiler_params=params(16),
        name="gather",
    )(in_plane(back))
    partial = pl.pallas_call(
        combine_kernel,
        out_shape=pltpu.VMEM(states.shape, BF16),
        in_specs=[VMEM, VMEM],
        out_specs=VMEM,
        compiler_params=params(16),
        name="combine",
    )(near(table), along_z(summed))
    added = partial.astype(F32) + swap(partial).astype(F32)
    return (states.astype(F32) + added).astype(BF16)


def solution(mesh):
    grid = Mesh(mesh.devices.reshape(*AXES, 2), ("y", "z", "x", "tensor"))
    group = ("y", "z", "x")
    placed = (
        P(group, None),
        P(),
        P(),
        P(group, None, "tensor"),
        P(group, None, "tensor"),
        P(group, "tensor", None),
        P(group, None),
        P(group, None),
        P(group, None),
    )
    return jax.shard_map(
        per_device, mesh=grid, in_specs=placed, out_specs=P(group, None), check_vma=False
    )
```

```python
import functools

import jax
import jax.numpy as jnp
import numpy as np
from jax import lax
from jax.experimental import pallas as pl
from jax.experimental.pallas import tpu as pltpu
from jax.sharding import PartitionSpec as P


SWAP = ((0, 1), (1, 0))
AXES = (4, 8, 4)
SIDE = 8
MIB = 1 << 20
BF16 = jnp.bfloat16
F32 = jnp.float32
VMEM = pl.BlockSpec(memory_space=pltpu.VMEM)
ANY = pl.BlockSpec(memory_space=pl.ANY)


def swap(x):
    return lax.ppermute(x, "tensor", SWAP)


def dot(a, b):
    return jnp.dot(a, b, preferred_element_type=F32)


def iota(shape, dim):
    return lax.broadcasted_iota(jnp.int32, shape, dim)


def slot_keys(own, tokens):
    _, zs, xs = AXES
    pairs = xs // 2
    core = lax.axis_index("tensor")
    shape = (SIDE, own, SIDE, tokens)
    outer, inner = iota(shape, 0), iota(shape, 2)
    z = jnp.where(core == 0, outer, inner)
    plane = jnp.where(core == 0, inner, outer)
    expert = (plane // pairs * zs + z) * pairs + plane % pairs
    key = expert * (2 * own) + iota(shape, 1) + core * own
    return key.reshape(SIDE * own * SIDE, tokens)


def stage_groups():
    ys, zs, xs = AXES
    flat = np.arange(ys * zs * xs * 2).reshape(ys, zs, xs // 2, 2, 2)
    first = (
        flat[..., 0].transpose(0, 2, 3, 1).reshape(-1, zs),
        flat[..., 1].transpose(1, 3, 0, 2).reshape(-1, ys * xs // 2),
    )
    second = (
        flat[..., 0].transpose(1, 0, 2, 3).reshape(-1, ys * xs),
        flat[..., 1].transpose(0, 2, 1, 3).reshape(-1, 2 * zs),
    )
    return tuple(np.concatenate(part).tolist() for part in (first, second))


def slot_numbers(own, ids, pos, keep):
    return jnp.where(keep[...] > 0, ids[...] * (2 * own) + pos[...], -1)


def dispatch_kernel(own, *refs):
    sources, (normed_out, send), targets, sems = refs[:5], refs[5:7], refs[7:12], refs[12]
    copies = [
        pltpu.make_async_copy(source, target, sems.at[n])
        for n, (source, target) in enumerate(zip(sources, targets))
    ]
    for copy in copies:
        copy.start()
    states, gain, ids, pos, keep = targets
    tokens = states.shape[0]
    for copy in copies[2:]:
        copy.wait()
    slots = slot_numbers(own, ids, pos, keep)
    key = slot_keys(own, tokens)
    hit = (key == slots[0:1, :]) | (key == slots[1:2, :])
    pick = jnp.where(hit, 1.0, 0.0).astype(BF16)
    for copy in copies[:2]:
        copy.wait()
    values = states[...].astype(F32)
    mean = jnp.mean(values * values, axis=-1, keepdims=True)
    normed = (values * lax.rsqrt(mean + 1e-06) * gain[...][None, :]).astype(BF16)
    normed_out[...] = normed
    send[...] = dot(pick, normed).astype(BF16)


def regroup_kernel(own, arrived, send):
    count = SIDE * own * SIDE
    shape = (SIDE, own, SIDE, count)
    source = (iota(shape, 2) * own + iota(shape, 1)) * SIDE + iota(shape, 0)
    pick = (source == iota(shape, 3)).reshape(count, count)
    rows = dot(jnp.where(pick, 1.0, 0.0).astype(BF16), arrived[...]).astype(BF16)
    size = own * SIDE
    for e in range(SIDE):
        for h in range(2):
            send[(2 * e + h) * size : (2 * e + h + 1) * size, :] = rows[e * size : (e + 1) * size, :]


def gather_kernel(own, partial, send):
    count = SIDE * own * SIDE
    shape = (SIDE, own, SIDE, 2 * count)
    holder = (iota(shape, 2) * 2 * own + iota(shape, 1)) * SIDE + iota(shape, 0)
    column = iota(shape, 3)
    pick = ((column == holder) | (column == holder + own * SIDE)).reshape(count, 2 * count)
    send[...] = dot(jnp.where(pick, 1.0, 0.0).astype(BF16), partial[...]).astype(BF16)


def weigh(own, normed, router, ids, pos, keep, table):
    tokens = normed.shape[0]
    experts = router.shape[0]
    logits = lax.dot_general(
        router[...], normed[...], (((1,), (1,)), ((), ())), preferred_element_type=F32
    )
    expert = iota((experts, tokens), 0)
    score = []
    for k in range(2):
        chosen = jnp.sum(jnp.where(expert == ids[k : k + 1, :], logits, 0.0), axis=0, keepdims=True)
        score.append(1.0 / (1.0 + jnp.exp(-chosen)))
    total = score[0] + score[1]
    slots = slot_numbers(own, ids, pos, keep)
    key = slot_keys(own, tokens)
    share = jnp.where(key == slots[0:1, :], score[0] / total, 0.0)
    share = share + jnp.where(key == slots[1:2, :], score[1] / total, 0.0)
    share = share.T
    high = share.astype(BF16)
    table[0] = high
    table[1] = (share - high.astype(F32)).astype(BF16)


def expert_kernel(own, rows, *refs):
    theirs, gate_mine, distant, routing = refs[:3], refs[3], refs[4:6], refs[6:11]
    back, table, hidden, up_mine, down_mine, sems = refs[11:]
    width = rows.shape[1]
    part = gate_mine.shape[1]
    block = 512
    copies = [
        pltpu.make_async_copy(source, target, sems.at[n])
        for n, (source, target) in enumerate(zip(distant, (up_mine, down_mine)))
    ]
    for copy in copies:
        copy.start()
    weigh(own, *routing, table)

    def hide(gates, ups, at):
        for n in range(part // block):
            cols = slice(n * block, (n + 1) * block)
            gate = dot(rows[...], gates[:, cols])
            up = dot(rows[...], ups[:, cols])
            hidden[:, at + n * block : at + (n + 1) * block] = (
                gate / (1.0 + jnp.exp(-gate)) * up
            ).astype(BF16)

    hide(theirs[0], theirs[1], 0)
    copies[0].wait()
    hide(gate_mine, up_mine, part)
    copies[1].wait()
    for n in range(width // block):
        cols = slice(n * block, (n + 1) * block)
        total = dot(hidden[:, :part], theirs[2][:, cols])
        total = total + dot(hidden[:, part:], down_mine[:, cols])
        back[:, cols] = total.astype(BF16)


def combine_kernel(table, returned, partial):
    partial[...] = (dot(table[0], returned[...]) + dot(table[1], returned[...])).astype(BF16)


def near(x):
    return pltpu.with_memory_space_constraint(x, pltpu.VMEM)


def far(x):
    return pltpu.with_memory_space_constraint(x, pltpu.HBM)


def params(mib):
    return pltpu.CompilerParams(vmem_limit_bytes=mib * MIB)


def per_device(states, norm_gain, router, w_gate, w_up, w_down, expert_ids, slot_pos, keep_mask):
    tokens, width = states.shape
    experts = router.shape[1]
    own = max(2, 5 * tokens // (2 * experts) + 1) // 2
    part = w_gate.shape[2]
    once = own * experts
    rows = pltpu.VMEM((once, width), BF16)
    twice = pltpu.VMEM((2 * once, width), BF16)
    mine = (w_gate[0], w_up[0], w_down[0])
    theirs = []
    for w in (w_gate, w_up, w_down):
        theirs.append(swap(w)[0])
    routing = (expert_ids.T, slot_pos.T, keep_mask.T)

    first, second = stage_groups()

    def exchange(x, groups):
        cut = x.reshape(len(groups[0]), -1, width)
        cut = lax.all_to_all(
            cut, ("expert", "tensor"), 0, 0, axis_index_groups=groups, tiled=True
        )
        return cut.reshape(x.shape)

    loaded = (states, norm_gain, *routing)
    normed, send = pl.pallas_call(
        functools.partial(dispatch_kernel, own),
        out_shape=(pltpu.VMEM(states.shape, BF16), rows),
        in_specs=[ANY] * 5,
        out_specs=(VMEM, VMEM),
        scratch_shapes=[pltpu.VMEM(x.shape, x.dtype) for x in loaded]
        + [pltpu.SemaphoreType.DMA((5,))],
        compiler_params=params(16),
        name="dispatch",
    )(*map(far, loaded))
    column, *theirs = lax.optimization_barrier((exchange(send, first), *theirs))
    spread = pl.pallas_call(
        functools.partial(regroup_kernel, own),
        out_shape=twice,
        in_specs=[VMEM],
        out_specs=VMEM,
        compiler_params=params(16),
        name="regroup",
    )(near(column))
    back, table = pl.pallas_call(
        functools.partial(expert_kernel, own),
        out_shape=(twice, pltpu.VMEM((2, tokens, once), BF16)),
        in_specs=[VMEM] * 5 + [ANY] * 2 + [VMEM] * 5,
        out_specs=(VMEM, VMEM),
        scratch_shapes=[
            pltpu.VMEM((2 * once, 2 * part), BF16),
            pltpu.VMEM((width, part), BF16),
            pltpu.VMEM((part, width), BF16),
            pltpu.SemaphoreType.DMA((2,)),
        ],
        compiler_params=params(40),
        cost_estimate=pl.CostEstimate(
            flops=24 * once * width * part, bytes_accessed=20 * 10**6, transcendentals=0
        ),
        name="experts",
    )(
        near(exchange(spread, second)),
        *map(near, (*theirs, mine[0])),
        *map(far, mine[1:]),
        near(normed),
        router.T,
        *routing,
    )
    summed = pl.pallas_call(
        functools.partial(gather_kernel, own),
        out_shape=rows,
        in_specs=[VMEM],
        out_specs=VMEM,
        compiler_params=params(16),
        name="gather",
    )(near(exchange(back, second)))
    partial = pl.pallas_call(
        combine_kernel,
        out_shape=pltpu.VMEM(states.shape, BF16),
        in_specs=[VMEM, VMEM],
        out_specs=VMEM,
        compiler_params=params(16),
        name="combine",
    )(near(table), near(exchange(summed, first)))
    added = partial.astype(F32) + swap(partial).astype(F32)
    return (states.astype(F32) + added).astype(BF16)


def solution(mesh):
    placed = (
        P("expert", None),
        P(),
        P(),
        P("expert", None, "tensor"),
        P("expert", None, "tensor"),
        P("expert", "tensor", None),
        P("expert", None),
        P("expert", None),
        P("expert", None),
    )

    return jax.shard_map(
        per_device, mesh=mesh, in_specs=placed, out_specs=P("expert", None), check_vma=False
    )
```

```python
import functools

import jax
import jax.numpy as jnp
import numpy as np
from jax import lax
from jax.experimental import pallas as pl
from jax.experimental.pallas import tpu as pltpu
from jax.sharding import PartitionSpec as P


SWAP = ((0, 1), (1, 0))
AXES = (4, 8, 4)
SIDE = 8
MIB = 1 << 20
BF16 = jnp.bfloat16
F32 = jnp.float32
VMEM = pl.BlockSpec(memory_space=pltpu.VMEM)
ANY = pl.BlockSpec(memory_space=pl.ANY)


def swap(x):
    return lax.ppermute(x, "tensor", SWAP)


def dot(a, b):
    return jnp.dot(a, b, preferred_element_type=F32)


def iota(shape, dim):
    return lax.broadcasted_iota(jnp.int32, shape, dim)


def slot_keys(own, tokens):
    _, zs, xs = AXES
    pairs = xs // 2
    core = lax.axis_index("tensor")
    shape = (SIDE, own, SIDE, tokens)
    outer, inner = iota(shape, 0), iota(shape, 2)
    z = jnp.where(core == 1, outer, inner)
    plane = jnp.where(core == 1, inner, outer)
    expert = (plane // pairs * zs + z) * pairs + plane % pairs
    key = expert * (2 * own) + iota(shape, 1) + core * own
    return key.reshape(SIDE * own * SIDE, tokens)


def stage_groups():
    ys, zs, xs = AXES
    flat = np.arange(ys * zs * xs * 2).reshape(ys, zs, xs // 2, 2, 2)
    first = (
        flat[..., 1].transpose(0, 2, 3, 1).reshape(-1, zs),
        flat[..., 0].transpose(1, 3, 0, 2).reshape(-1, ys * xs // 2),
    )
    second = (
        flat[..., 1].transpose(1, 0, 2, 3).reshape(-1, ys * xs),
        flat[..., 0].transpose(0, 2, 1, 3).reshape(-1, 2 * zs),
    )
    return tuple(np.concatenate(part).tolist() for part in (first, second))


def slot_numbers(own, ids, pos, keep):
    return jnp.where(keep[...] > 0, ids[...] * (2 * own) + pos[...], -1)


def dispatch_kernel(own, *refs):
    sources, (normed_out, send), targets, sems = refs[:5], refs[5:7], refs[7:12], refs[12]
    copies = [
        pltpu.make_async_copy(source, target, sems.at[n])
        for n, (source, target) in enumerate(zip(sources, targets))
    ]
    for copy in copies:
        copy.start()
    states, gain, ids, pos, keep = targets
    tokens = states.shape[0]
    for copy in copies[2:]:
        copy.wait()
    slots = slot_numbers(own, ids, pos, keep)
    key = slot_keys(own, tokens)
    hit = (key == slots[0:1, :]) | (key == slots[1:2, :])
    pick = jnp.where(hit, 1.0, 0.0).astype(BF16)
    for copy in copies[:2]:
        copy.wait()
    values = states[...].astype(F32)
    mean = jnp.mean(values * values, axis=-1, keepdims=True)
    normed = (values * lax.rsqrt(mean + 1e-06) * gain[...][None, :]).astype(BF16)
    normed_out[...] = normed
    send[...] = dot(pick, normed).astype(BF16)


def regroup_kernel(own, arrived, send):
    count = SIDE * own * SIDE
    shape = (SIDE, own, SIDE, count)
    source = (iota(shape, 2) * own + iota(shape, 1)) * SIDE + iota(shape, 0)
    pick = (source == iota(shape, 3)).reshape(count, count)
    rows = dot(jnp.where(pick, 1.0, 0.0).astype(BF16), arrived[...]).astype(BF16)
    size = own * SIDE
    for e in range(SIDE):
        for h in range(2):
            send[(2 * e + h) * size : (2 * e + h + 1) * size, :] = rows[e * size : (e + 1) * size, :]


def gather_kernel(own, partial, send):
    count = SIDE * own * SIDE
    shape = (SIDE, own, SIDE, 2 * count)
    holder = (iota(shape, 2) * 2 * own + iota(shape, 1)) * SIDE + iota(shape, 0)
    column = iota(shape, 3)
    pick = ((column == holder) | (column == holder + own * SIDE)).reshape(count, 2 * count)
    send[...] = dot(jnp.where(pick, 1.0, 0.0).astype(BF16), partial[...]).astype(BF16)


def weigh(own, normed, router, ids, pos, keep, table):
    tokens = normed.shape[0]
    experts = router.shape[0]
    logits = lax.dot_general(
        router[...], normed[...], (((1,), (1,)), ((), ())), preferred_element_type=F32
    )
    expert = iota((experts, tokens), 0)
    score = []
    for k in range(2):
        chosen = jnp.sum(jnp.where(expert == ids[k : k + 1, :], logits, 0.0), axis=0, keepdims=True)
        score.append(1.0 / (1.0 + jnp.exp(-chosen)))
    total = score[0] + score[1]
    slots = slot_numbers(own, ids, pos, keep)
    key = slot_keys(own, tokens)
    share = jnp.where(key == slots[0:1, :], score[0] / total, 0.0)
    share = share + jnp.where(key == slots[1:2, :], score[1] / total, 0.0)
    share = share.T
    high = share.astype(BF16)
    table[0] = high
    table[1] = (share - high.astype(F32)).astype(BF16)


def expert_kernel(own, rows, *refs):
    theirs, gate_mine, distant, routing = refs[:3], refs[3], refs[4:6], refs[6:11]
    back, table, hidden, up_mine, down_mine, sems = refs[11:]
    width = rows.shape[1]
    part = gate_mine.shape[1]
    block = 512
    copies = [
        pltpu.make_async_copy(source, target, sems.at[n])
        for n, (source, target) in enumerate(zip(distant, (up_mine, down_mine)))
    ]
    for copy in copies:
        copy.start()
    weigh(own, *routing, table)

    def hide(gates, ups, at):
        for n in range(part // block):
            cols = slice(n * block, (n + 1) * block)
            gate = dot(rows[...], gates[:, cols])
            up = dot(rows[...], ups[:, cols])
            hidden[:, at + n * block : at + (n + 1) * block] = (
                gate / (1.0 + jnp.exp(-gate)) * up
            ).astype(BF16)

    hide(theirs[0], theirs[1], 0)
    copies[0].wait()
    hide(gate_mine, up_mine, part)
    copies[1].wait()
    for n in range(width // block):
        cols = slice(n * block, (n + 1) * block)
        total = dot(hidden[:, :part], theirs[2][:, cols])
        total = total + dot(hidden[:, part:], down_mine[:, cols])
        back[:, cols] = total.astype(BF16)


def combine_kernel(table, returned, partial):
    partial[...] = (dot(table[0], returned[...]) + dot(table[1], returned[...])).astype(BF16)


def near(x):
    return pltpu.with_memory_space_constraint(x, pltpu.VMEM)


def far(x):
    return pltpu.with_memory_space_constraint(x, pltpu.HBM)


def params(mib):
    return pltpu.CompilerParams(vmem_limit_bytes=mib * MIB)


def per_device(states, norm_gain, router, w_gate, w_up, w_down, expert_ids, slot_pos, keep_mask):
    tokens, width = states.shape
    experts = router.shape[1]
    own = max(2, 5 * tokens // (2 * experts) + 1) // 2
    part = w_gate.shape[2]
    once = own * experts
    rows = pltpu.VMEM((once, width), BF16)
    twice = pltpu.VMEM((2 * once, width), BF16)
    mine = (w_gate[0], w_up[0], w_down[0])
    theirs = []
    for w in (w_gate, w_up, w_down):
        theirs.append(swap(w)[0])
    routing = (expert_ids.T, slot_pos.T, keep_mask.T)

    first, second = stage_groups()

    def exchange(x, groups):
        cut = x.reshape(len(groups[0]), -1, width)
        cut = lax.all_to_all(
            cut, ("expert", "tensor"), 0, 0, axis_index_groups=groups, tiled=True
        )
        return cut.reshape(x.shape)

    loaded = (states, norm_gain, *routing)
    normed, send = pl.pallas_call(
        functools.partial(dispatch_kernel, own),
        out_shape=(pltpu.VMEM(states.shape, BF16), rows),
        in_specs=[ANY] * 5,
        out_specs=(VMEM, VMEM),
        scratch_shapes=[pltpu.VMEM(x.shape, x.dtype) for x in loaded]
        + [pltpu.SemaphoreType.DMA((5,))],
        compiler_params=params(16),
        name="dispatch",
    )(*map(far, loaded))
    column, *theirs = lax.optimization_barrier((exchange(send, first), *theirs))
    spread = pl.pallas_call(
        functools.partial(regroup_kernel, own),
        out_shape=twice,
        in_specs=[VMEM],
        out_specs=VMEM,
        compiler_params=params(16),
        name="regroup",
    )(near(column))
    back, table = pl.pallas_call(
        functools.partial(expert_kernel, own),
        out_shape=(twice, pltpu.VMEM((2, tokens, once), BF16)),
        in_specs=[VMEM] * 5 + [ANY] * 2 + [VMEM] * 5,
        out_specs=(VMEM, VMEM),
        scratch_shapes=[
            pltpu.VMEM((2 * once, 2 * part), BF16),
            pltpu.VMEM((width, part), BF16),
            pltpu.VMEM((part, width), BF16),
            pltpu.SemaphoreType.DMA((2,)),
        ],
        compiler_params=params(40),
        cost_estimate=pl.CostEstimate(
            flops=24 * once * width * part, bytes_accessed=20 * 10**6, transcendentals=0
        ),
        name="experts",
    )(
        near(exchange(spread, second)),
        *map(near, (*theirs, mine[0])),
        *map(far, mine[1:]),
        near(normed),
        router.T,
        *routing,
    )
    summed = pl.pallas_call(
        functools.partial(gather_kernel, own),
        out_shape=rows,
        in_specs=[VMEM],
        out_specs=VMEM,
        compiler_params=params(16),
        name="gather",
    )(near(exchange(back, second)))
    partial = pl.pallas_call(
        combine_kernel,
        out_shape=pltpu.VMEM(states.shape, BF16),
        in_specs=[VMEM, VMEM],
        out_specs=VMEM,
        compiler_params=params(16),
        name="combine",
    )(near(table), near(exchange(summed, first)))
    added = partial.astype(F32) + swap(partial).astype(F32)
    return (states.astype(F32) + added).astype(BF16)


def solution(mesh):
    placed = (
        P("expert", None),
        P(),
        P(),
        P("expert", None, "tensor"),
        P("expert", None, "tensor"),
        P("expert", "tensor", None),
        P("expert", None),
        P("expert", None),
        P("expert", None),
    )

    return jax.shard_map(
        per_device, mesh=mesh, in_specs=placed, out_specs=P("expert", None), check_vma=False
    )
```

```python
import functools

import jax
import jax.numpy as jnp
import numpy as np
from jax import lax
from jax.experimental import pallas as pl
from jax.experimental.pallas import tpu as pltpu
from jax.sharding import PartitionSpec as P


SWAP = ((0, 1), (1, 0))
AXES = (4, 8, 4)
SIDE = 8
MIB = 1 << 20
BF16 = jnp.bfloat16
F32 = jnp.float32
VMEM = pl.BlockSpec(memory_space=pltpu.VMEM)
ANY = pl.BlockSpec(memory_space=pl.ANY)


def swap(x):
    return lax.ppermute(x, "tensor", SWAP)


def dot(a, b):
    return jnp.dot(a, b, preferred_element_type=F32)


def iota(shape, dim):
    return lax.broadcasted_iota(jnp.int32, shape, dim)


def slot_keys(own, tokens):
    _, zs, xs = AXES
    pairs = xs // 2
    core = lax.axis_index("tensor")
    shape = (SIDE, own, SIDE, tokens)
    outer, inner = iota(shape, 0), iota(shape, 2)
    z = jnp.where(core == 1, outer, inner)
    plane = jnp.where(core == 1, inner, outer)
    expert = (plane // pairs * zs + z) * pairs + plane % pairs
    key = expert * (2 * own) + iota(shape, 1) + core * own
    return key.reshape(SIDE * own * SIDE, tokens)


def stage_groups():
    ys, zs, xs = AXES
    flat = np.arange(ys * zs * xs * 2).reshape(ys, zs, xs // 2, 2, 2)
    first = (
        flat[..., 1].transpose(0, 2, 3, 1).reshape(-1, zs),
        flat[..., 0].transpose(1, 3, 0, 2).reshape(-1, ys * xs // 2),
    )
    second = (
        flat[..., 1].transpose(1, 0, 2, 3).reshape(-1, ys * xs),
        flat[..., 0].transpose(0, 2, 1, 3).reshape(-1, 2 * zs),
    )
    return tuple(np.concatenate(part).tolist() for part in (first, second))


def slot_numbers(own, ids, pos, keep):
    return jnp.where(keep[...] > 0, ids[...] * (2 * own) + pos[...], -1)


def dispatch_kernel(own, *refs):
    sources, (normed_out, send), targets, sems = refs[:5], refs[5:7], refs[7:12], refs[12]
    copies = [
        pltpu.make_async_copy(source, target, sems.at[n])
        for n, (source, target) in enumerate(zip(sources, targets))
    ]
    for copy in copies:
        copy.start()
    states, gain, ids, pos, keep = targets
    tokens = states.shape[0]
    for copy in copies[2:]:
        copy.wait()
    slots = slot_numbers(own, ids, pos, keep)
    key = slot_keys(own, tokens)
    hit = (key == slots[0:1, :]) | (key == slots[1:2, :])
    pick = jnp.where(hit, 1.0, 0.0).astype(BF16)
    for copy in copies[:2]:
        copy.wait()
    values = states[...].astype(F32)
    mean = jnp.mean(values * values, axis=-1, keepdims=True)
    normed = (values * lax.rsqrt(mean + 1e-06) * gain[...][None, :]).astype(BF16)
    normed_out[...] = normed
    send[...] = dot(pick, normed).astype(BF16)


def regroup_kernel(own, arrived, send):
    count = SIDE * own * SIDE
    shape = (SIDE, own, SIDE, count)
    source = (iota(shape, 2) * own + iota(shape, 1)) * SIDE + iota(shape, 0)
    pick = (source == iota(shape, 3)).reshape(count, count)
    rows = dot(jnp.where(pick, 1.0, 0.0).astype(BF16), arrived[...]).astype(BF16)
    size = own * SIDE
    for e in range(SIDE):
        for h in range(2):
            send[(2 * e + h) * size : (2 * e + h + 1) * size, :] = rows[e * size : (e + 1) * size, :]


def gather_kernel(own, partial, send):
    count = SIDE * own * SIDE
    shape = (SIDE, own, SIDE, 2 * count)
    holder = (iota(shape, 2) * 2 * own + iota(shape, 1)) * SIDE + iota(shape, 0)
    column = iota(shape, 3)
    pick = ((column == holder) | (column == holder + own * SIDE)).reshape(count, 2 * count)
    send[...] = dot(jnp.where(pick, 1.0, 0.0).astype(BF16), partial[...]).astype(BF16)


def weigh(own, normed, router, ids, pos, keep, table):
    tokens = normed.shape[0]
    experts = router.shape[0]
    logits = lax.dot_general(
        router[...], normed[...], (((1,), (1,)), ((), ())), preferred_element_type=F32
    )
    expert = iota((experts, tokens), 0)
    chosen = [
        jnp.sum(jnp.where(expert == ids[k : k + 1, :], logits, 0.0), axis=0, keepdims=True)
        for k in range(2)
    ]
    low = jnp.minimum(jnp.minimum(chosen[0], chosen[1]), 0.0)
    inverse = [jnp.exp(low) + jnp.exp(low - c) for c in chosen]
    total = inverse[0] + inverse[1]
    slots = slot_numbers(own, ids, pos, keep)
    key = slot_keys(own, tokens)
    share = jnp.where(key == slots[0:1, :], inverse[1] / total, 0.0)
    share = share + jnp.where(key == slots[1:2, :], inverse[0] / total, 0.0)
    share = share.T
    high = share.astype(BF16)
    table[0] = high
    table[1] = (share - high.astype(F32)).astype(BF16)


def expert_kernel(own, rows, *refs):
    theirs, gate_mine, distant, routing = refs[:3], refs[3], refs[4:6], refs[6:11]
    back, table, hidden, up_mine, down_mine, sems = refs[11:]
    width = rows.shape[1]
    part = gate_mine.shape[1]
    block = 512
    copies = [
        pltpu.make_async_copy(source, target, sems.at[n])
        for n, (source, target) in enumerate(zip(distant, (up_mine, down_mine)))
    ]
    for copy in copies:
        copy.start()
    weigh(own, *routing, table)

    def hide(gates, ups, at):
        for n in range(part // block):
            cols = slice(n * block, (n + 1) * block)
            gate = dot(rows[...], gates[:, cols])
            up = dot(rows[...], ups[:, cols])
            hidden[:, at + n * block : at + (n + 1) * block] = (
                gate / (1.0 + jnp.exp(-gate)) * up
            ).astype(BF16)

    hide(theirs[0], theirs[1], 0)
    copies[0].wait()
    hide(gate_mine, up_mine, part)
    copies[1].wait()
    for n in range(width // block):
        cols = slice(n * block, (n + 1) * block)
        total = dot(hidden[:, :part], theirs[2][:, cols])
        total = total + dot(hidden[:, part:], down_mine[:, cols])
        back[:, cols] = total.astype(BF16)


def combine_kernel(table, returned, partial):
    partial[...] = (dot(table[0], returned[...]) + dot(table[1], returned[...])).astype(BF16)


def near(x):
    return pltpu.with_memory_space_constraint(x, pltpu.VMEM)


def far(x):
    return pltpu.with_memory_space_constraint(x, pltpu.HBM)


def params(mib):
    return pltpu.CompilerParams(vmem_limit_bytes=mib * MIB)


def per_device(states, norm_gain, router, w_gate, w_up, w_down, expert_ids, slot_pos, keep_mask):
    tokens, width = states.shape
    experts = router.shape[1]
    own = max(2, 5 * tokens // (2 * experts) + 1) // 2
    part = w_gate.shape[2]
    once = own * experts
    rows = pltpu.VMEM((once, width), BF16)
    twice = pltpu.VMEM((2 * once, width), BF16)
    mine = (w_gate[0], w_up[0], w_down[0])
    theirs = []
    for w in (w_gate, w_up, w_down):
        theirs.append(swap(w)[0])
    routing = (expert_ids.T, slot_pos.T, keep_mask.T)

    first, second = stage_groups()

    def exchange(x, groups):
        cut = x.reshape(len(groups[0]), -1, width)
        cut = lax.all_to_all(
            cut, ("expert", "tensor"), 0, 0, axis_index_groups=groups, tiled=True
        )
        return cut.reshape(x.shape)

    loaded = (states, norm_gain, *routing)
    normed, send = pl.pallas_call(
        functools.partial(dispatch_kernel, own),
        out_shape=(pltpu.VMEM(states.shape, BF16), rows),
        in_specs=[ANY] * 5,
        out_specs=(VMEM, VMEM),
        scratch_shapes=[pltpu.VMEM(x.shape, x.dtype) for x in loaded]
        + [pltpu.SemaphoreType.DMA((5,))],
        compiler_params=params(16),
        name="dispatch",
    )(*map(far, loaded))
    column, *theirs = lax.optimization_barrier((exchange(send, first), *theirs))
    spread = pl.pallas_call(
        functools.partial(regroup_kernel, own),
        out_shape=twice,
        in_specs=[VMEM],
        out_specs=VMEM,
        compiler_params=params(16),
        name="regroup",
    )(near(column))
    back, table = pl.pallas_call(
        functools.partial(expert_kernel, own),
        out_shape=(twice, pltpu.VMEM((2, tokens, once), BF16)),
        in_specs=[VMEM] * 5 + [ANY] * 2 + [VMEM] * 5,
        out_specs=(VMEM, VMEM),
        scratch_shapes=[
            pltpu.VMEM((2 * once, 2 * part), BF16),
            pltpu.VMEM((width, part), BF16),
            pltpu.VMEM((part, width), BF16),
            pltpu.SemaphoreType.DMA((2,)),
        ],
        compiler_params=params(40),
        cost_estimate=pl.CostEstimate(
            flops=24 * once * width * part, bytes_accessed=20 * 10**6, transcendentals=0
        ),
        name="experts",
    )(
        near(exchange(spread, second)),
        *map(near, (*theirs, mine[0])),
        *map(far, mine[1:]),
        near(normed),
        router.T,
        *routing,
    )
    summed = pl.pallas_call(
        functools.partial(gather_kernel, own),
        out_shape=rows,
        in_specs=[VMEM],
        out_specs=VMEM,
        compiler_params=params(16),
        name="gather",
    )(near(exchange(back, second)))
    partial = pl.pallas_call(
        combine_kernel,
        out_shape=pltpu.VMEM(states.shape, BF16),
        in_specs=[VMEM, VMEM],
        out_specs=VMEM,
        compiler_params=params(16),
        name="combine",
    )(near(table), near(exchange(summed, first)))
    added = partial.astype(F32) + swap(partial).astype(F32)
    return (states.astype(F32) + added).astype(BF16)


def solution(mesh):
    placed = (
        P("expert", None),
        P(),
        P(),
        P("expert", None, "tensor"),
        P("expert", None, "tensor"),
        P("expert", "tensor", None),
        P("expert", None),
        P("expert", None),
        P("expert", None),
    )

    return jax.shard_map(
        per_device, mesh=mesh, in_specs=placed, out_specs=P("expert", None), check_vma=False
    )
```

```python
import functools

import jax
import jax.numpy as jnp
import numpy as np
from jax import lax
from jax.experimental import pallas as pl
from jax.experimental.pallas import tpu as pltpu
from jax.sharding import PartitionSpec as P


SWAP = ((0, 1), (1, 0))
AXES = (4, 8, 4)
SIDE = 8
MIB = 1 << 20
BF16 = jnp.bfloat16
F32 = jnp.float32
VMEM = pl.BlockSpec(memory_space=pltpu.VMEM)
ANY = pl.BlockSpec(memory_space=pl.ANY)


def swap(x):
    return lax.ppermute(x, "tensor", SWAP)


def dot(a, b):
    return jnp.dot(a, b, preferred_element_type=F32)


def iota(shape, dim):
    return lax.broadcasted_iota(jnp.int32, shape, dim)


def slot_keys(own, tokens):
    _, zs, xs = AXES
    pairs = xs // 2
    core = lax.axis_index("tensor")
    shape = (SIDE, own, SIDE, tokens)
    outer, inner = iota(shape, 0), iota(shape, 2)
    z = jnp.where(core == 1, outer, inner)
    plane = jnp.where(core == 1, inner, outer)
    expert = (plane // pairs * zs + z) * pairs + plane % pairs
    key = expert * (2 * own) + iota(shape, 1) + core * own
    return key.reshape(SIDE * own * SIDE, tokens)


def stage_groups():
    ys, zs, xs = AXES
    flat = np.arange(ys * zs * xs * 2).reshape(ys, zs, xs // 2, 2, 2)
    first = (
        flat[..., 1].transpose(0, 2, 3, 1).reshape(-1, zs),
        flat[..., 0].transpose(1, 3, 0, 2).reshape(-1, ys * xs // 2),
    )
    second = (
        flat[..., 1].transpose(1, 0, 2, 3).reshape(-1, ys * xs),
        flat[..., 0].transpose(0, 2, 1, 3).reshape(-1, 2 * zs),
    )
    return tuple(np.concatenate(part).tolist() for part in (first, second))


def slot_numbers(own, ids, pos, keep):
    return jnp.where(keep[...] > 0, ids[...] * (2 * own) + pos[...], -1)


def dispatch_kernel(own, *refs):
    sources, (normed_out, send), targets, sems = refs[:5], refs[5:7], refs[7:12], refs[12]
    copies = [
        pltpu.make_async_copy(source, target, sems.at[n])
        for n, (source, target) in enumerate(zip(sources, targets))
    ]
    for copy in copies:
        copy.start()
    states, gain, ids, pos, keep = targets
    tokens = states.shape[0]
    for copy in copies[2:]:
        copy.wait()
    slots = slot_numbers(own, ids, pos, keep)
    key = slot_keys(own, tokens)
    hit = (key == slots[0:1, :]) | (key == slots[1:2, :])
    pick = jnp.where(hit, 1.0, 0.0).astype(BF16)
    for copy in copies[:2]:
        copy.wait()
    values = states[...].astype(F32)
    mean = jnp.mean(values * values, axis=-1, keepdims=True)
    normed = (values * lax.rsqrt(mean + 1e-06) * gain[...][None, :]).astype(BF16)
    normed_out[...] = normed
    send[...] = dot(pick, normed).astype(BF16)


def regroup_kernel(own, arrived, send):
    count = SIDE * own * SIDE
    shape = (SIDE, own, SIDE, count)
    source = (iota(shape, 2) * own + iota(shape, 1)) * SIDE + iota(shape, 0)
    pick = (source == iota(shape, 3)).reshape(count, count)
    rows = dot(jnp.where(pick, 1.0, 0.0).astype(BF16), arrived[...]).astype(BF16)
    size = own * SIDE
    for e in range(SIDE):
        for h in range(2):
            send[(2 * e + h) * size : (2 * e + h + 1) * size, :] = rows[e * size : (e + 1) * size, :]


def gather_kernel(own, partial, send):
    count = SIDE * own * SIDE
    size = own * SIDE
    sums = []
    for e in range(SIDE):
        one = partial[2 * e * size : (2 * e + 1) * size, :].astype(F32)
        two = partial[(2 * e + 1) * size : (2 * e + 2) * size, :].astype(F32)
        sums.append(one + two)
    rows = jnp.concatenate(sums, axis=0).astype(BF16)
    shape = (SIDE, own, SIDE, count)
    source = (iota(shape, 2) * own + iota(shape, 1)) * SIDE + iota(shape, 0)
    pick = (source == iota(shape, 3)).reshape(count, count)
    send[...] = dot(jnp.where(pick, 1.0, 0.0).astype(BF16), rows).astype(BF16)


def weigh(own, normed, router, ids, pos, keep, table):
    tokens = normed.shape[0]
    experts = router.shape[0]
    logits = lax.dot_general(
        router[...], normed[...], (((1,), (1,)), ((), ())), preferred_element_type=F32
    )
    expert = iota((experts, tokens), 0)
    chosen = [
        jnp.sum(jnp.where(expert == ids[k : k + 1, :], logits, 0.0), axis=0, keepdims=True)
        for k in range(2)
    ]
    low = jnp.minimum(jnp.minimum(chosen[0], chosen[1]), 0.0)
    inverse = [jnp.exp(low) + jnp.exp(low - c) for c in chosen]
    total = inverse[0] + inverse[1]
    slots = slot_numbers(own, ids, pos, keep)
    key = slot_keys(own, tokens)
    share = jnp.where(key == slots[0:1, :], inverse[1] / total, 0.0)
    share = share + jnp.where(key == slots[1:2, :], inverse[0] / total, 0.0)
    share = share.T
    high = share.astype(BF16)
    table[0] = high
    table[1] = (share - high.astype(F32)).astype(BF16)


def expert_kernel(own, rows, *refs):
    theirs, gate_mine, distant, routing = refs[:3], refs[3], refs[4:6], refs[6:11]
    back, table, hidden, up_mine, down_mine, sems = refs[11:]
    width = rows.shape[1]
    part = gate_mine.shape[1]
    block = 512
    copies = [
        pltpu.make_async_copy(source, target, sems.at[n])
        for n, (source, target) in enumerate(zip(distant, (up_mine, down_mine)))
    ]
    for copy in copies:
        copy.start()
    weigh(own, *routing, table)

    def hide(gates, ups, at):
        for n in range(part // block):
            cols = slice(n * block, (n + 1) * block)
            gate = dot(rows[...], gates[:, cols])
            up = dot(rows[...], ups[:, cols])
            hidden[:, at + n * block : at + (n + 1) * block] = (
                gate / (1.0 + jnp.exp(-gate)) * up
            ).astype(BF16)

    hide(theirs[0], theirs[1], 0)
    copies[0].wait()
    hide(gate_mine, up_mine, part)
    copies[1].wait()
    for n in range(width // block):
        cols = slice(n * block, (n + 1) * block)
        total = dot(hidden[:, :part], theirs[2][:, cols])
        total = total + dot(hidden[:, part:], down_mine[:, cols])
        back[:, cols] = total.astype(BF16)


def combine_kernel(table, returned, partial):
    partial[...] = (dot(table[0], returned[...]) + dot(table[1], returned[...])).astype(BF16)


def near(x):
    return pltpu.with_memory_space_constraint(x, pltpu.VMEM)


def far(x):
    return pltpu.with_memory_space_constraint(x, pltpu.HBM)


def params(mib):
    return pltpu.CompilerParams(vmem_limit_bytes=mib * MIB)


def per_device(states, norm_gain, router, w_gate, w_up, w_down, expert_ids, slot_pos, keep_mask):
    tokens, width = states.shape
    experts = router.shape[1]
    own = max(2, 5 * tokens // (2 * experts) + 1) // 2
    part = w_gate.shape[2]
    once = own * experts
    rows = pltpu.VMEM((once, width), BF16)
    twice = pltpu.VMEM((2 * once, width), BF16)
    mine = (w_gate[0], w_up[0], w_down[0])
    theirs = []
    for w in (w_gate, w_up, w_down):
        theirs.append(swap(w)[0])
    routing = (expert_ids.T, slot_pos.T, keep_mask.T)

    first, second = stage_groups()

    def exchange(x, groups):
        cut = x.reshape(len(groups[0]), -1, width)
        cut = lax.all_to_all(
            cut, ("expert", "tensor"), 0, 0, axis_index_groups=groups, tiled=True
        )
        return cut.reshape(x.shape)

    loaded = (states, norm_gain, *routing)
    normed, send = pl.pallas_call(
        functools.partial(dispatch_kernel, own),
        out_shape=(pltpu.VMEM(states.shape, BF16), rows),
        in_specs=[ANY] * 5,
        out_specs=(VMEM, VMEM),
        scratch_shapes=[pltpu.VMEM(x.shape, x.dtype) for x in loaded]
        + [pltpu.SemaphoreType.DMA((5,))],
        compiler_params=params(16),
        name="dispatch",
    )(*map(far, loaded))
    column, *theirs = lax.optimization_barrier((exchange(send, first), *theirs))
    spread = pl.pallas_call(
        functools.partial(regroup_kernel, own),
        out_shape=twice,
        in_specs=[VMEM],
        out_specs=VMEM,
        compiler_params=params(16),
        name="regroup",
    )(near(column))
    back, table = pl.pallas_call(
        functools.partial(expert_kernel, own),
        out_shape=(twice, pltpu.VMEM((2, tokens, once), BF16)),
        in_specs=[VMEM] * 5 + [ANY] * 2 + [VMEM] * 5,
        out_specs=(VMEM, VMEM),
        scratch_shapes=[
            pltpu.VMEM((2 * once, 2 * part), BF16),
            pltpu.VMEM((width, part), BF16),
            pltpu.VMEM((part, width), BF16),
            pltpu.SemaphoreType.DMA((2,)),
        ],
        compiler_params=params(40),
        cost_estimate=pl.CostEstimate(
            flops=24 * once * width * part, bytes_accessed=20 * 10**6, transcendentals=0
        ),
        name="experts",
    )(
        near(exchange(spread, second)),
        *map(near, (*theirs, mine[0])),
        *map(far, mine[1:]),
        near(normed),
        router.T,
        *routing,
    )
    summed = pl.pallas_call(
        functools.partial(gather_kernel, own),
        out_shape=rows,
        in_specs=[VMEM],
        out_specs=VMEM,
        compiler_params=params(16),
        name="gather",
    )(near(exchange(back, second)))
    partial = pl.pallas_call(
        combine_kernel,
        out_shape=pltpu.VMEM(states.shape, BF16),
        in_specs=[VMEM, VMEM],
        out_specs=VMEM,
        compiler_params=params(16),
        name="combine",
    )(near(table), near(exchange(summed, first)))
    added = partial.astype(F32) + swap(partial).astype(F32)
    return (states.astype(F32) + added).astype(BF16)


def solution(mesh):
    placed = (
        P("expert", None),
        P(),
        P(),
        P("expert", None, "tensor"),
        P("expert", None, "tensor"),
        P("expert", "tensor", None),
        P("expert", None),
        P("expert", None),
        P("expert", None),
    )

    return jax.shard_map(
        per_device, mesh=mesh, in_specs=placed, out_specs=P("expert", None), check_vma=False
    )
```
